32 devices in a mesh: ep: 32 (over z, y, x, core).
Axes of the slice: x: 2, y: 2, z: 4, core: 2. Of those that a mesh axis runs over, the one named last changes fastest.
Arguments:
- tokens: bfloat16 [512, 7168], P('ep'), may hold values from -6 to 6
- router_weight: bfloat16 [7168, 16], replicated, may hold values from -0.0625 to 0.0625
- expert_ids: int32 [512, 8], P('ep'), may hold values from 0 to 15, as said below
- gate_proj: bfloat16 [32, 2, 7168, 256], P('ep'), may hold values from -0.0625 to 0.0625
- up_proj: bfloat16 [32, 2, 7168, 256], P('ep'), may hold values from -0.0625 to 0.0625
- down_proj: bfloat16 [32, 2, 256, 7168], P('ep'), may hold values from -0.1875 to 0.1875
Outputs:
- mixed: bfloat16 [512, 7168], P('ep')
- load_excess: float32 [16], replicated
The draws below stay inside these ranges and needn't reach their ends.
Inputs may be any that keep to these rules, and one draw needn't show every extreme that they name: `expert_ids`: each token names 8 different experts, all in different groups (expert e is in group e // 2). Among the 16 tokens of any one index of ep, at most 16 choices name experts of any one group, and some group is named by exactly 16 of them.
All inputs are finite; a program needn't handle non-finite values.
Results may differ from the reference program's by a relative error of at most 0.015.
Values may be sent and summed in bfloat16 or wider, within the bound.
A program may use at most 128 MiB of HBM per device.

```python
import jax
import jax.numpy as jnp
from jax import lax

D = 7168
TOP = 8
FF = 1024
SPLIT = 4
EXP_GRP = 2
TOK_DEV = 16
GROUPS = 8
EXPERTS = 16
FF_DEV = 256
TOKENS = 512
PAIR_CAP = 16
N_EP = 32


def device_routes(key):
    perm_key, ticket_key, local_key = jax.random.split(key, 3)
    assigned = TOK_DEV * TOP
    group_order = jax.random.permutation(perm_key, GROUPS).astype(jnp.int32)
    tickets = jax.random.permutation(ticket_key, (GROUPS - 1) * PAIR_CAP).astype(jnp.int32)
    taken_tickets = tickets[:assigned - PAIR_CAP]
    per_group = jnp.zeros((GROUPS,), jnp.int32).at[0].set(PAIR_CAP)
    per_group = per_group.at[1 + taken_tickets // PAIR_CAP].add(1)
    run_ends = jnp.cumsum(per_group)
    position = jnp.arange(assigned, dtype=jnp.int32)
    rank_of = jnp.sum((position[:, None] >= run_ends[None, :]).astype(jnp.int32), axis=1)
    groups_hit = group_order[rank_of]
    local_expert = jax.random.randint(local_key, (assigned,), 0, EXP_GRP, dtype=jnp.int32)
    experts = groups_hit * EXP_GRP + local_expert
    return experts.reshape(TOP, TOK_DEV).T


def draw_expert_ids(key, part):
    block_keys = jax.random.split(key, N_EP)
    blocks = jax.vmap(device_routes)(block_keys)
    return blocks.reshape(TOKENS, TOP).astype(jnp.int32)


def shard_levels(stream_key, shape, cuts, least, top_value):
    gain, own = 1.0, jax.random.fold_in(stream_key, 6)
    for axis_at, shards_of in cuts:
        heights = jnp.exp(jax.random.uniform(jax.random.fold_in(own, axis_at), (shards_of,), jnp.float32, least / len(cuts), top_value / len(cuts)))
        gain = gain * jnp.repeat(heights, shape[axis_at] // shards_of).reshape([-1 if axis == axis_at else 1 for axis in range(len(shape))])
    return gain


def gaussian(own_key, shape, scale, most, cuts=(), kind=jnp.bfloat16):
    values = scale * jax.random.normal(own_key, shape, jnp.float32)
    if cuts:
        values = values * shard_levels(own_key, shape, cuts, -0.22, 0.18)
    return jnp.clip(values, -most, most).astype(kind)


def setup_inputs(seed: int = 0) -> dict:
    key_of = jax.random.split(jax.random.key(seed), 7)
    tokens = gaussian(key_of[0], (TOKENS, D), 1.0, 6.0, ((0, 32),))
    router_weight = gaussian(key_of[1], (D, EXPERTS), D ** -0.5, 0.0625)
    expert_ids = draw_expert_ids(jax.random.fold_in(key_of[6], 71), 0)
    gate_proj = gaussian(key_of[3], (N_EP, EXP_GRP, D, FF_DEV), D ** -0.5, 0.0625, ((0, 32),))
    up_proj = gaussian(key_of[4], (N_EP, EXP_GRP, D, FF_DEV), D ** -0.5, 0.0625, ((0, 32),))
    down_proj = gaussian(key_of[5], (N_EP, EXP_GRP, FF_DEV, D), FF ** -0.5, 0.1875, ((0, 32),))
    return dict(tokens=tokens, router_weight=router_weight, expert_ids=expert_ids, gate_proj=gate_proj, up_proj=up_proj, down_proj=down_proj)


route_scale = 2.5
block_rows = 16


def routing_gates(tokens, router_weight, expert_ids):
    logits = jnp.dot(tokens, router_weight, preferred_element_type=jnp.float32)
    scores = jax.nn.sigmoid(logits)
    picked = jnp.take_along_axis(scores, expert_ids, axis=1)
    return route_scale * picked / jnp.sum(picked, axis=1, keepdims=True)


def expert_rows(token_rows, gate_weight, up_weight, down_weight):
    gate_act = jnp.dot(token_rows, gate_weight, preferred_element_type=jnp.float32)
    up_act = jnp.dot(token_rows, up_weight, preferred_element_type=jnp.float32)
    hidden = (jax.nn.silu(gate_act) * up_act).astype(jnp.bfloat16)
    return jnp.dot(hidden, down_weight, preferred_element_type=jnp.float32).astype(jnp.bfloat16)


def reference(tokens, router_weight, expert_ids, gate_proj, up_proj, down_proj):
    gate_weights = routing_gates(tokens, router_weight, expert_ids).reshape(-1)
    chosen = expert_ids.reshape(-1).astype(jnp.int32)
    row_limit = (N_EP * PAIR_CAP + block_rows - 1) // block_rows * block_rows
    offsets = jnp.arange(block_rows, dtype=jnp.int32)

    def run_expert(summed, expert, gate_weight, up_weight, down_weight):
        is_hit = chosen == expert
        hit_count = jnp.sum(is_hit.astype(jnp.int32))
        where_hit = jnp.nonzero(is_hit, size=row_limit, fill_value=0)[0].astype(jnp.int32)

        def one_block(block_index, running):
            first_row = (block_index * block_rows).astype(jnp.int32)
            picked_rows = lax.dynamic_slice_in_dim(where_hit, first_row, block_rows)
            owners = picked_rows // TOP
            result = lax.optimization_barrier(expert_rows(tokens[owners], gate_weight, up_weight, down_weight))
            weight = jnp.where(first_row + offsets < hit_count, gate_weights[picked_rows], 0.0)
            return running.at[owners].add(weight[:, None] * result.astype(jnp.float32))

        blocks = (hit_count + block_rows - 1) // block_rows
        return lax.fori_loop(0, blocks, one_block, summed)

    def one_group(summed, inputs):
        gate_group, up_group, down_group, group = inputs
        for local in range(EXP_GRP):
            gate_weight = jnp.transpose(gate_group[:, local], (1, 0, 2)).reshape(D, FF)
            up_weight = jnp.transpose(up_group[:, local], (1, 0, 2)).reshape(D, FF)
            down_weight = down_group[:, local].reshape(FF, D)
            expert = (group * EXP_GRP + local).astype(jnp.int32)
            summed = run_expert(summed, expert, gate_weight, up_weight, down_weight)
        return summed, None

    gate_groups = gate_proj.reshape(GROUPS, SPLIT, EXP_GRP, D, FF_DEV)
    up_groups = up_proj.reshape(GROUPS, SPLIT, EXP_GRP, D, FF_DEV)
    down_groups = down_proj.reshape(GROUPS, SPLIT, EXP_GRP, FF_DEV, D)
    group_index = jnp.arange(GROUPS, dtype=jnp.int32)
    initial = jnp.zeros((TOKENS, D), jnp.float32)
    summed = lax.scan(one_group, initial, (gate_groups, up_groups, down_groups, group_index))[0]
    expert_index = jnp.arange(EXPERTS, dtype=jnp.int32)
    expert_loads = jnp.sum((chosen[:, None] == expert_index[None, :]).astype(jnp.int32), axis=0)
    load_excess = (expert_loads - TOKENS * TOP // EXPERTS).astype(jnp.float32)
    return summed.astype(jnp.bfloat16), load_excess
```

```python
import jax
import jax.numpy as jnp
from jax import lax
from jax.sharding import PartitionSpec as P

SPLIT = 4


route_scale = 2.5


def per_device(tokens, router_weight, expert_ids, gate_proj, up_proj, down_proj):
    experts = router_weight.shape[1]
    held = gate_proj.shape[1]
    fanout = expert_ids.shape[1]
    features = tokens.shape[1]
    logits = jnp.dot(tokens, router_weight, preferred_element_type=jnp.float32)
    scores = jax.nn.sigmoid(logits)
    hits = expert_ids[:, :, None] == jnp.arange(experts, dtype=jnp.int32)
    picked = jnp.sum(jnp.where(hits, scores[:, None, :], 0.0), axis=2)
    gates = route_scale * picked / jnp.sum(picked, axis=1, keepdims=True)
    dense = jnp.sum(jnp.where(hits, gates[:, :, None], 0.0), axis=1)
    named = jnp.sum(hits.astype(jnp.float32), axis=1)
    small = lax.all_gather(jnp.concatenate([dense, named], axis=1), "ep", axis=0, tiled=True)
    rows = lax.all_gather(tokens, "ep", axis=0, tiled=True)
    load = jnp.sum(small[:, experts:], axis=0)
    load_excess = load - float(small.shape[0] * fanout // experts)
    group = lax.axis_index("ep") // SPLIT
    weights = lax.dynamic_slice_in_dim(small, group * held, held, axis=1)
    parts = []
    for slot in range(held):
        gate_act = jnp.dot(rows, gate_proj[0, slot], preferred_element_type=jnp.float32)
        up_act = jnp.dot(rows, up_proj[0, slot], preferred_element_type=jnp.float32)
        hidden = jax.nn.silu(gate_act) * up_act * weights[:, slot : slot + 1]
        parts.append(hidden.astype(jnp.bfloat16))
    hidden = jnp.concatenate(parts, axis=1)
    down = down_proj[0].reshape(-1, features)
    partial = jnp.dot(hidden, down, preferred_element_type=jnp.float32).astype(jnp.bfloat16)
    mixed = lax.psum_scatter(partial, "ep", scatter_dimension=0, tiled=True)
    return mixed, load_excess


def solution(mesh):
    in_specs = (
        P("ep", None),
        P(),
        P("ep", None),
        P("ep", None, None, None),
        P("ep", None, None, None),
        P("ep", None, None, None),
    )
    out_specs = (P("ep", None), P())
    return jax.shard_map(
        per_device, mesh=mesh, in_specs=in_specs, out_specs=out_specs, check_vma=False
    )
```

```python
import functools

import jax
import jax.numpy as jnp
from jax import lax
from jax.experimental import pallas as pl
from jax.experimental.pallas import tpu as pltpu
from jax.sharding import PartitionSpec as P

SPLIT = 4
MESH = pl.DeviceIdType.MESH
LANES = 128
VMEM_LIMIT = 67_000_000


route_scale = 2.5


def kernel(
    chunk,
    tok_hbm, small_hbm, gate_hbm, up_hbm, down_hbm,
    out_ref, load_ref,
    rows, small, wg, wu, wd, acc_g, acc_u, hid, part,
    r0, q0, r1, q1, r2, q2, r3,
    send, recv, ssend, srecv, local,
):
    deep = rows.shape[0]
    tok = rows.shape[4]
    features = rows.shape[5]
    held = wg.shape[0]
    ff = wg.shape[2]
    total_rows = deep * 8 * tok
    pair = 2 * chunk
    count = features // pair
    me = lax.axis_index("ep")
    core = lax.rem(me, 2)
    x = lax.rem(me // 2, 2)
    y = lax.rem(me // 4, 2)
    z = me // 8

    def index(zi, yi, xi, ci):
        return ((zi * 2 + yi) * 2 + xi) * 2 + ci

    core_peer = index(z, y, x, 1 - core)
    x_peer = index(z, y, 1 - x, core)
    y_peer = index(z, 1 - y, x, core)
    z_at = [lax.rem(z + o, deep) for o in range(1, deep)]
    z_peers = [index(zi, y, x, core) for zi in z_at]
    hops = deep - 1

    fetch = [
        pltpu.make_async_copy(tok_hbm, rows.at[z, y, x, core], local.at[0]),
        pltpu.make_async_copy(small_hbm, small.at[z, y, x, core], local.at[1]),
        pltpu.make_async_copy(gate_hbm.at[0], wg, local.at[2]),
        pltpu.make_async_copy(up_hbm.at[0], wu, local.at[3]),
        pltpu.make_async_copy(down_hbm.at[0], wd, local.at[4]),
    ]
    for copy in fetch:
        copy.start()

    barrier = pltpu.get_barrier_semaphore()
    peers = [core_peer, x_peer, y_peer] + z_peers
    for peer in peers:
        pl.semaphore_signal(barrier, inc=1, device_id=(peer,), device_id_type=MESH)
    pl.semaphore_wait(barrier, len(peers))

    def remote(src, dst, ss, rs, peer):
        return pltpu.make_async_remote_copy(
            src_ref=src, dst_ref=dst, send_sem=ss, recv_sem=rs,
            device_id=(peer,), device_id_type=MESH,
        )

    def span(p):
        return pl.ds(pl.multiple_of(p * pair, pair), pair)

    def span_a(p):
        return pl.ds(pl.multiple_of(p * pair, chunk), chunk)

    def span_b(p):
        return pl.ds(pl.multiple_of(p * pair + chunk, chunk), chunk)

    def put(p, slot, src, dst, peer):
        return remote(src, dst, send.at[p, slot], recv.at[p, slot], peer)

    def same(ref, at, p, slot, peer):
        view = ref.at[at]
        return put(p, slot, view, view, peer)

    every = slice(None)

    def gather_z(p):
        return [
            same(rows, (z, y, x, core, every, span(p)), p, o, z_peers[o]) for o in range(hops)
        ]

    def gather_1(p):
        return [
            same(rows, (every, y, x, core, every, span_a(p)), p, hops, x_peer),
            same(rows, (every, y, x, core, every, span_b(p)), p, hops + 1, y_peer),
        ]

    def gather_2(p):
        return [
            same(rows, (every, y, every, core, every, span_a(p)), p, hops + 2, y_peer),
            same(rows, (every, every, x, core, every, span_b(p)), p, hops + 3, x_peer),
        ]

    def gather_core(p):
        return [
            same(rows, (every, every, every, core, every, span(p)), p, hops + 4, core_peer)
        ]

    def small_copy(at, slot, peer):
        view = small.at[at]
        return remote(view, view, ssend.at[slot], srecv.at[slot], peer)

    small_z = [small_copy((z, y, x, core), o, z_peers[o]) for o in range(hops)]
    small_x = [small_copy((every, y, x, core), hops, x_peer)]
    small_y = [small_copy((every, y, every, core), hops + 1, y_peer)]
    small_core = [small_copy((every, every, every, core), hops + 2, core_peer)]

    def start(copies):
        for copy in copies:
            copy.start()

    def wait(copies):
        for copy in copies:
            copy.wait()

    fetch[0].wait()
    fetch[1].wait()

    def first(p, carry):
        start(gather_z(p))
        return carry

    start(gather_z(0))
    start(small_z)
    lax.fori_loop(1, count, first, 0)
    acc_g[...] = jnp.zeros_like(acc_g)
    acc_u[...] = jnp.zeros_like(acc_u)
    fetch[2].wait()
    fetch[3].wait()

    def gather_step(t, carry):
        @pl.when(t < count)
        def _():
            wait(gather_z(t))
            start(gather_1(t))

        @pl.when(jnp.logical_and(t >= 1, t < count + 1))
        def _():
            wait(gather_1(t - 1))
            start(gather_2(t - 1))

        @pl.when(jnp.logical_and(t >= 2, t < count + 2))
        def _():
            wait(gather_2(t - 2))
            start(gather_core(t - 2))

        @pl.when(t >= 3)
        def _():
            p = t - 3
            wait(gather_core(p))
            block = rows[:, :, :, :, :, span(p)].reshape(total_rows, pair)
            for slot in range(held):
                acc_g[slot] += jnp.dot(
                    block, wg[slot, span(p), :], preferred_element_type=jnp.float32
                )
                acc_u[slot] += jnp.dot(
                    block, wu[slot, span(p), :], preferred_element_type=jnp.float32
                )

        @pl.when(t == 0)
        def _():
            wait(small_z)
            start(small_x)

        @pl.when(t == 1)
        def _():
            wait(small_x)
            start(small_y)

        @pl.when(t == 2)
        def _():
            wait(small_y)
            start(small_core)

        return carry

    lax.fori_loop(0, count + 3, gather_step, 0)
    wait(small_core)
    fetch[4].wait()

    table = small[...].reshape(total_rows, LANES)
    load_ref[...] = jnp.broadcast_to(jnp.sum(table, axis=0, keepdims=True), load_ref.shape)
    lane = lax.broadcasted_iota(jnp.int32, (total_rows, LANES), 1)
    for slot in range(held):
        mine = lane == me // SPLIT * held + slot
        weight = jnp.sum(jnp.where(mine, table, 0.0), axis=1, keepdims=True)
        gate_act = acc_g[slot]
        hidden = gate_act / (1.0 + jnp.exp(-gate_act)) * acc_u[slot] * weight
        hid[:, slot * ff : (slot + 1) * ff] = hidden.astype(hid.dtype)

    base = hops + 5

    def fold_core(p):
        return [
            put(p, base, part.at[:, :, :, 1 - core, :, span(p)], r0.at[:, :, :, :, span(p)], core_peer)
        ]

    def fold_1(p):
        a, b = span_a(p), span_b(p)
        return [
            put(p, base + 1, q0.at[:, 1 - y, :, :, a], r1.at[:, :, :, a], y_peer),
            put(p, base + 2, q0.at[:, :, 1 - x, :, b], r1.at[:, :, :, b], x_peer),
        ]

    def fold_2(p):
        a, b = span_a(p), span_b(p)
        return [
            put(p, base + 3, q1.at[:, 1 - x, :, a], r2.at[:, :, a], x_peer),
            put(p, base + 4, q1.at[:, 1 - y, :, b], r2.at[:, :, b], y_peer),
        ]

    def fold_z(p):
        return [
            put(p, base + 5 + o, q2.at[z_at[o], :, span(p)], r3.at[o, :, span(p)], z_peers[o])
            for o in range(hops)
        ]

    def add(a, b):
        return (a.astype(jnp.float32) + b.astype(jnp.float32)).astype(jnp.bfloat16)

    def fold_step(t, carry):
        @pl.when(t < count)
        def _():
            s = span(t)
            down = wd[:, :, s].reshape(held * ff, pair)
            made = jnp.dot(hid[...], down, preferred_element_type=jnp.float32)
            part[:, :, :, :, :, s] = made.astype(jnp.bfloat16).reshape(
                deep, 2, 2, 2, tok, pair
            )
            start(fold_core(t))

        @pl.when(jnp.logical_and(t >= 1, t < count + 1))
        def _():
            p = t - 1
            s = span(p)
            wait(fold_core(p))
            q0[:, :, :, :, s] = add(part[:, :, :, core, :, s], r0[:, :, :, :, s])
            start(fold_1(p))

        @pl.when(jnp.logical_and(t >= 2, t < count + 2))
        def _():
            p = t - 2
            a, b = span_a(p), span_b(p)
            wait(fold_1(p))
            q1[:, :, :, a] = add(q0[:, y, :, :, a], r1[:, :, :, a])
            q1[:, :, :, b] = add(q0[:, :, x, :, b], r1[:, :, :, b])
            start(fold_2(p))

        @pl.when(jnp.logical_and(t >= 3, t < count + 3))
        def _():
            p = t - 3
            a, b = span_a(p), span_b(p)
            wait(fold_2(p))
            q2[:, :, a] = add(q1[:, x, :, a], r2[:, :, a])
            q2[:, :, b] = add(q1[:, y, :, b], r2[:, :, b])
            start(fold_z(p))

        @pl.when(t >= 4)
        def _():
            p = t - 4
            s = span(p)
            wait(fold_z(p))
            total = q2[z, :, s].astype(jnp.float32)
            for o in range(hops):
                total = total + r3[o, :, s].astype(jnp.float32)
            out_ref[:, s] = total.astype(out_ref.dtype)

        return carry

    lax.fori_loop(0, count + 4, fold_step, 0)


def exchange(tokens, small, gate_proj, up_proj, down_proj, devices, chunk):
    tok, features = tokens.shape
    held, _, ff = gate_proj.shape[1:]
    deep = devices // 8
    total_rows = devices * tok
    count = features // (2 * chunk)
    hops = deep - 1
    slots = 2 * (hops + 5)
    bf16, f32 = jnp.bfloat16, jnp.float32
    hbm = pl.BlockSpec(memory_space=pl.ANY)
    vmem = pl.BlockSpec(memory_space=pltpu.VMEM)
    return pl.pallas_call(
        functools.partial(kernel, chunk),
        out_shape=(
            jax.ShapeDtypeStruct((tok, features), bf16),
            jax.ShapeDtypeStruct((8, LANES), f32),
        ),
        in_specs=[hbm] * 5,
        out_specs=(vmem, vmem),
        scratch_shapes=[
            pltpu.VMEM((deep, 2, 2, 2, tok, features), bf16),
            pltpu.VMEM((deep, 2, 2, 2, tok, LANES), f32),
            pltpu.VMEM((held, features, ff), bf16),
            pltpu.VMEM((held, features, ff), bf16),
            pltpu.VMEM((held, ff, features), bf16),
            pltpu.VMEM((held, total_rows, ff), f32),
            pltpu.VMEM((held, total_rows, ff), f32),
            pltpu.VMEM((total_rows, held * ff), bf16),
            pltpu.VMEM((deep, 2, 2, 2, tok, features), bf16),
            pltpu.VMEM((deep, 2, 2, tok, features), bf16),
            pltpu.VMEM((deep, 2, 2, tok, features), bf16),
            pltpu.VMEM((deep, 2, tok, features), bf16),
            pltpu.VMEM((deep, 2, tok, features), bf16),
            pltpu.VMEM((deep, tok, features), bf16),
            pltpu.VMEM((deep, tok, features), bf16),
            pltpu.VMEM((max(hops, 1), tok, features), bf16),
            pltpu.SemaphoreType.DMA((count, slots)),
            pltpu.SemaphoreType.DMA((count, slots)),
            pltpu.SemaphoreType.DMA((hops + 3,)),
            pltpu.SemaphoreType.DMA((hops + 3,)),
            pltpu.SemaphoreType.DMA((5,)),
        ],
        compiler_params=pltpu.CompilerParams(
            collective_id=0, has_side_effects=True, vmem_limit_bytes=VMEM_LIMIT
        ),
    )(tokens, small, gate_proj, up_proj, down_proj)


def chunk_width(devices, tokens, expert_ids, router_weight, gate_proj):
    tok, features = tokens.shape
    held, _, ff = gate_proj.shape[1:]
    row_bytes = devices * tok * features * 2
    need = 4 * row_bytes + 3 * held * features * ff * 2 + devices * tok * held * ff * 10
    fits = need + (2 << 20) <= VMEM_LIMIT and 2 * router_weight.shape[1] <= LANES
    if devices % 8 or tok % 16 or ff % LANES or not fits:
        return 0
    for width in (CHUNK, 2 * LANES, LANES):
        if features % (2 * width) == 0:
            return width
    return 0


CHUNK = 512


def per_device(tokens, router_weight, expert_ids, gate_proj, up_proj, down_proj):
    experts = router_weight.shape[1]
    held = gate_proj.shape[1]
    fanout = expert_ids.shape[1]
    features = tokens.shape[1]
    logits = jnp.dot(tokens, router_weight, preferred_element_type=jnp.float32)
    scores = jax.nn.sigmoid(logits)
    hits = expert_ids[:, :, None] == jnp.arange(experts, dtype=jnp.int32)
    picked = jnp.sum(jnp.where(hits, scores[:, None, :], 0.0), axis=2)
    gates = route_scale * picked / jnp.sum(picked, axis=1, keepdims=True)
    dense = jnp.sum(jnp.where(hits, gates[:, :, None], 0.0), axis=1)
    named = jnp.sum(hits.astype(jnp.float32), axis=1)
    devices = lax.axis_size("ep")
    chunk = chunk_width(devices, tokens, expert_ids, router_weight, gate_proj)
    mean_load = float(devices * tokens.shape[0] * fanout // experts)
    both = jnp.concatenate([dense, named], axis=1)
    if chunk:
        both = jnp.pad(both, ((0, 0), (0, LANES - 2 * experts)))
        mixed, loads = exchange(
            tokens, both, gate_proj, up_proj, down_proj, devices, chunk
        )
        return mixed, loads[0, experts : 2 * experts] - mean_load
    small = lax.all_gather(both, "ep", axis=0, tiled=True)
    rows = lax.all_gather(tokens, "ep", axis=0, tiled=True)
    load = jnp.sum(small[:, experts:], axis=0)
    load_excess = load - mean_load
    group = lax.axis_index("ep") // SPLIT
    weights = lax.dynamic_slice_in_dim(small, group * held, held, axis=1)
    parts = []
    for slot in range(held):
        gate_act = jnp.dot(rows, gate_proj[0, slot], preferred_element_type=jnp.float32)
        up_act = jnp.dot(rows, up_proj[0, slot], preferred_element_type=jnp.float32)
        hidden = jax.nn.silu(gate_act) * up_act * weights[:, slot : slot + 1]
        parts.append(hidden.astype(jnp.bfloat16))
    hidden = jnp.concatenate(parts, axis=1)
    down = down_proj[0].reshape(-1, features)
    partial = jnp.dot(hidden, down, preferred_element_type=jnp.float32).astype(jnp.bfloat16)
    mixed = lax.psum_scatter(partial, "ep", scatter_dimension=0, tiled=True)
    return mixed, load_excess


def solution(mesh):
    in_specs = (
        P("ep", None),
        P(),
        P("ep", None),
        P("ep", None, None, None),
        P("ep", None, None, None),
        P("ep", None, None, None),
    )
    out_specs = (P("ep", None), P())
    return jax.shard_map(
        per_device, mesh=mesh, in_specs=in_specs, out_specs=out_specs, check_vma=False
    )
```

```python
import functools

import jax
import jax.numpy as jnp
from jax import lax
from jax.experimental import pallas as pl
from jax.experimental.pallas import tpu as pltpu
from jax.sharding import PartitionSpec as P

SPLIT = 4
MESH = pl.DeviceIdType.MESH
LANES = 128
VMEM_LIMIT = 67_000_000


route_scale = 2.5


def kernel(
    chunk, mean_load,
    tok_hbm, small_hbm, gate_hbm, up_hbm, down_hbm,
    out_ref, load_ref,
    rows, small, wg, wu, wd, acc_g, acc_u, hid, part,
    r0, q0, r1, q1, r2, q2, r3,
    send, recv, ssend, srecv, local,
):
    deep = rows.shape[0]
    tok = rows.shape[4]
    features = rows.shape[5]
    held = wg.shape[0]
    ff = wg.shape[2]
    total_rows = deep * 8 * tok
    pair = 2 * chunk
    count = features // pair
    me = lax.axis_index("ep")
    core = lax.rem(me, 2)
    x = lax.rem(me // 2, 2)
    y = lax.rem(me // 4, 2)
    z = me // 8

    def index(zi, yi, xi, ci):
        return ((zi * 2 + yi) * 2 + xi) * 2 + ci

    core_peer = index(z, y, x, 1 - core)
    x_peer = index(z, y, 1 - x, core)
    y_peer = index(z, 1 - y, x, core)
    z_at = [lax.rem(z + o, deep) for o in range(1, deep)]
    z_peers = [index(zi, y, x, core) for zi in z_at]
    hops = deep - 1

    fetch = [
        pltpu.make_async_copy(tok_hbm, rows.at[z, y, x, core], local.at[0]),
        pltpu.make_async_copy(small_hbm, small.at[z, y, x, core], local.at[1]),
        pltpu.make_async_copy(gate_hbm.at[0], wg, local.at[2]),
        pltpu.make_async_copy(up_hbm.at[0], wu, local.at[3]),
        pltpu.make_async_copy(down_hbm.at[0], wd, local.at[4]),
    ]
    for copy in fetch:
        copy.start()

    barrier = pltpu.get_barrier_semaphore()
    peers = [core_peer, x_peer, y_peer] + z_peers
    for peer in peers:
        pl.semaphore_signal(barrier, inc=1, device_id=(peer,), device_id_type=MESH)
    pl.semaphore_wait(barrier, len(peers))

    def remote(src, dst, ss, rs, peer):
        return pltpu.make_async_remote_copy(
            src_ref=src, dst_ref=dst, send_sem=ss, recv_sem=rs,
            device_id=(peer,), device_id_type=MESH,
        )

    def span(p):
        return pl.ds(pl.multiple_of(p * pair, pair), pair)

    def span_a(p):
        return pl.ds(pl.multiple_of(p * pair, chunk), chunk)

    def span_b(p):
        return pl.ds(pl.multiple_of(p * pair + chunk, chunk), chunk)

    def put(p, slot, src, dst, peer):
        return remote(src, dst, send.at[p, slot], recv.at[p, slot], peer)

    def same(ref, at, p, slot, peer):
        view = ref.at[at]
        return put(p, slot, view, view, peer)

    every = slice(None)

    def gather_z(p):
        return [
            same(rows, (z, y, x, core, every, span(p)), p, o, z_peers[o]) for o in range(hops)
        ]

    def gather_1(p):
        return [
            same(rows, (every, y, x, core, every, span_a(p)), p, hops, x_peer),
            same(rows, (every, y, x, core, every, span_b(p)), p, hops + 1, y_peer),
        ]

    def gather_2(p):
        return [
            same(rows, (every, y, every, core, every, span_a(p)), p, hops + 2, y_peer),
            same(rows, (every, every, x, core, every, span_b(p)), p, hops + 3, x_peer),
        ]

    def gather_core(p):
        return [
            same(rows, (every, every, every, core, every, span(p)), p, hops + 4, core_peer)
        ]

    def small_copy(at, slot, peer):
        view = small.at[at]
        return remote(view, view, ssend.at[slot], srecv.at[slot], peer)

    small_z = [small_copy((z, y, x, core), o, z_peers[o]) for o in range(hops)]
    small_x = [small_copy((every, y, x, core), hops, x_peer)]
    small_y = [small_copy((every, y, every, core), hops + 1, y_peer)]
    small_core = [small_copy((every, every, every, core), hops + 2, core_peer)]

    def start(copies):
        for copy in copies:
            copy.start()

    def wait(copies):
        for copy in copies:
            copy.wait()

    fetch[0].wait()
    fetch[1].wait()

    def first(p, carry):
        start(gather_z(p))
        return carry

    start(gather_z(0))
    start(small_z)
    lax.fori_loop(1, count, first, 0)
    acc_g[...] = jnp.zeros_like(acc_g)
    acc_u[...] = jnp.zeros_like(acc_u)

    def gather_step(t, carry):
        @pl.when(t < count)
        def _():
            wait(gather_z(t))
            start(gather_1(t))

        @pl.when(jnp.logical_and(t >= 1, t < count + 1))
        def _():
            wait(gather_1(t - 1))
            start(gather_2(t - 1))

        @pl.when(jnp.logical_and(t >= 2, t < count + 2))
        def _():
            wait(gather_2(t - 2))
            start(gather_core(t - 2))

        @pl.when(t >= 3)
        def _():
            p = t - 3

            @pl.when(p == 0)
            def _():
                fetch[2].wait()
                fetch[3].wait()

            wait(gather_core(p))
            block = rows[:, :, :, :, :, span(p)].reshape(total_rows, pair)
            for slot in range(held):
                acc_g[slot] += jnp.dot(
                    block, wg[slot, span(p), :], preferred_element_type=jnp.float32
                )
                acc_u[slot] += jnp.dot(
                    block, wu[slot, span(p), :], preferred_element_type=jnp.float32
                )

        @pl.when(t == 0)
        def _():
            wait(small_z)
            start(small_x)

        @pl.when(t == 1)
        def _():
            wait(small_x)
            start(small_y)

        @pl.when(t == 2)
        def _():
            wait(small_y)
            start(small_core)

        return carry

    lax.fori_loop(0, count + 3, gather_step, 0)
    wait(small_core)
    fetch[4].wait()

    table = small[...].reshape(total_rows, LANES)
    experts = load_ref.shape[1]
    load_ref[...] = jnp.sum(table, axis=0, keepdims=True)[:, :experts] - mean_load
    lane = lax.broadcasted_iota(jnp.int32, (total_rows, LANES), 1)
    for slot in range(held):
        mine = lane == load_ref.shape[1] + me // SPLIT * held + slot
        weight = jnp.sum(jnp.where(mine, table, 0.0), axis=1, keepdims=True)
        gate_act = acc_g[slot]
        hidden = gate_act / (1.0 + jnp.exp(-gate_act)) * acc_u[slot] * weight
        hid[:, slot * ff : (slot + 1) * ff] = hidden.astype(hid.dtype)

    base = hops + 5

    def fold_core(p):
        return [
            put(p, base, part.at[:, :, :, 1 - core, :, span(p)], r0.at[:, :, :, :, span(p)], core_peer)
        ]

    def fold_1(p):
        a, b = span_a(p), span_b(p)
        return [
            put(p, base + 1, q0.at[:, 1 - y, :, :, a], r1.at[:, :, :, a], y_peer),
            put(p, base + 2, q0.at[:, :, 1 - x, :, b], r1.at[:, :, :, b], x_peer),
        ]

    def fold_2(p):
        a, b = span_a(p), span_b(p)
        return [
            put(p, base + 3, q1.at[:, 1 - x, :, a], r2.at[:, :, a], x_peer),
            put(p, base + 4, q1.at[:, 1 - y, :, b], r2.at[:, :, b], y_peer),
        ]

    def fold_z(p):
        return [
            put(p, base + 5 + o, q2.at[z_at[o], :, span(p)], r3.at[o, :, span(p)], z_peers[o])
            for o in range(hops)
        ]

    def add(a, b):
        return (a.astype(jnp.float32) + b.astype(jnp.float32)).astype(jnp.bfloat16)

    def fold_step(t, carry):
        @pl.when(t < count)
        def _():
            s = span(t)
            down = wd[:, :, s].reshape(held * ff, pair)
            made = jnp.dot(hid[...], down, preferred_element_type=jnp.float32)
            part[:, :, :, :, :, s] = made.astype(jnp.bfloat16).reshape(
                deep, 2, 2, 2, tok, pair
            )
            start(fold_core(t))

        @pl.when(jnp.logical_and(t >= 1, t < count + 1))
        def _():
            p = t - 1
            s = span(p)
            wait(fold_core(p))
            q0[:, :, :, :, s] = add(part[:, :, :, core, :, s], r0[:, :, :, :, s])
            start(fold_1(p))

        @pl.when(jnp.logical_and(t >= 2, t < count + 2))
        def _():
            p = t - 2
            a, b = span_a(p), span_b(p)
            wait(fold_1(p))
            q1[:, :, :, a] = add(q0[:, y, :, :, a], r1[:, :, :, a])
            q1[:, :, :, b] = add(q0[:, :, x, :, b], r1[:, :, :, b])
            start(fold_2(p))

        @pl.when(jnp.logical_and(t >= 3, t < count + 3))
        def _():
            p = t - 3
            a, b = span_a(p), span_b(p)
            wait(fold_2(p))
            q2[:, :, a] = add(q1[:, x, :, a], r2[:, :, a])
            q2[:, :, b] = add(q1[:, y, :, b], r2[:, :, b])
            start(fold_z(p))

        @pl.when(t >= 4)
        def _():
            p = t - 4
            s = span(p)
            wait(fold_z(p))
            total = q2[z, :, s].astype(jnp.float32)
            for o in range(hops):
                total = total + r3[o, :, s].astype(jnp.float32)
            out_ref[:, s] = total.astype(out_ref.dtype)

        return carry

    lax.fori_loop(0, count + 4, fold_step, 0)


def exchange(tokens, small, gate_proj, up_proj, down_proj, devices, chunk, mean_load, experts):
    tok, features = tokens.shape
    held, _, ff = gate_proj.shape[1:]
    deep = devices // 8
    total_rows = devices * tok
    count = features // (2 * chunk)
    hops = deep - 1
    slots = 2 * (hops + 5)
    bf16, f32 = jnp.bfloat16, jnp.float32
    hbm = pl.BlockSpec(memory_space=pl.ANY)
    vmem = pl.BlockSpec(memory_space=pltpu.VMEM)
    return pl.pallas_call(
        functools.partial(kernel, chunk, mean_load),
        out_shape=(
            jax.ShapeDtypeStruct((tok, features), bf16),
            jax.ShapeDtypeStruct((1, experts), f32),
        ),
        in_specs=[hbm] * 5,
        out_specs=(vmem, vmem),
        scratch_shapes=[
            pltpu.VMEM((deep, 2, 2, 2, tok, features), bf16),
            pltpu.VMEM((deep, 2, 2, 2, tok, LANES), f32),
            pltpu.VMEM((held, features, ff), bf16),
            pltpu.VMEM((held, features, ff), bf16),
            pltpu.VMEM((held, ff, features), bf16),
            pltpu.VMEM((held, total_rows, ff), f32),
            pltpu.VMEM((held, total_rows, ff), f32),
            pltpu.VMEM((total_rows, held * ff), bf16),
            pltpu.VMEM((deep, 2, 2, 2, tok, features), bf16),
            pltpu.VMEM((deep, 2, 2, tok, features), bf16),
            pltpu.VMEM((deep, 2, 2, tok, features), bf16),
            pltpu.VMEM((deep, 2, tok, features), bf16),
            pltpu.VMEM((deep, 2, tok, features), bf16),
            pltpu.VMEM((deep, tok, features), bf16),
            pltpu.VMEM((deep, tok, features), bf16),
            pltpu.VMEM((max(hops, 1), tok, features), bf16),
            pltpu.SemaphoreType.DMA((count, slots)),
            pltpu.SemaphoreType.DMA((count, slots)),
            pltpu.SemaphoreType.DMA((hops + 3,)),
            pltpu.SemaphoreType.DMA((hops + 3,)),
            pltpu.SemaphoreType.DMA((5,)),
        ],
        compiler_params=pltpu.CompilerParams(
            collective_id=0, has_side_effects=True, vmem_limit_bytes=VMEM_LIMIT
        ),
    )(tokens, small, gate_proj, up_proj, down_proj)


def chunk_width(devices, tokens, expert_ids, router_weight, gate_proj):
    tok, features = tokens.shape
    held, _, ff = gate_proj.shape[1:]
    row_bytes = devices * tok * features * 2
    need = 4 * row_bytes + 3 * held * features * ff * 2 + devices * tok * held * ff * 10
    fits = need + (2 << 20) <= VMEM_LIMIT and 2 * router_weight.shape[1] <= LANES
    if devices % 8 or tok % 16 or ff % LANES or not fits:
        return 0
    for width in (CHUNK, 2 * LANES, LANES):
        if features % (2 * width) == 0:
            return width
    return 0


CHUNK = 512


def per_device(tokens, router_weight, expert_ids, gate_proj, up_proj, down_proj):
    experts = router_weight.shape[1]
    held = gate_proj.shape[1]
    fanout = expert_ids.shape[1]
    features = tokens.shape[1]
    logits = jnp.dot(tokens, router_weight, preferred_element_type=jnp.float32)
    scores = jax.nn.sigmoid(logits)
    hits = expert_ids[:, :, None] == jnp.arange(experts, dtype=jnp.int32)
    picked = jnp.sum(jnp.where(hits, scores[:, None, :], 0.0), axis=2)
    gates = route_scale * picked / jnp.sum(picked, axis=1, keepdims=True)
    dense = jnp.sum(jnp.where(hits, gates[:, :, None], 0.0), axis=1)
    named = jnp.sum(hits.astype(jnp.float32), axis=1)
    devices = lax.axis_size("ep")
    chunk = chunk_width(devices, tokens, expert_ids, router_weight, gate_proj)
    mean_load = float(devices * tokens.shape[0] * fanout // experts)
    both = jnp.concatenate([dense, named], axis=1)
    if chunk:
        both = jnp.concatenate([named, dense], axis=1)
        both = jnp.pad(both, ((0, 0), (0, LANES - 2 * experts)))
        mixed, loads = exchange(
            tokens, both, gate_proj, up_proj, down_proj, devices, chunk, mean_load, experts
        )
        return mixed, loads.reshape(-1)
    small = lax.all_gather(both, "ep", axis=0, tiled=True)
    rows = lax.all_gather(tokens, "ep", axis=0, tiled=True)
    load = jnp.sum(small[:, experts:], axis=0)
    load_excess = load - mean_load
    group = lax.axis_index("ep") // SPLIT
    weights = lax.dynamic_slice_in_dim(small, group * held, held, axis=1)
    parts = []
    for slot in range(held):
        gate_act = jnp.dot(rows, gate_proj[0, slot], preferred_element_type=jnp.float32)
        up_act = jnp.dot(rows, up_proj[0, slot], preferred_element_type=jnp.float32)
        hidden = jax.nn.silu(gate_act) * up_act * weights[:, slot : slot + 1]
        parts.append(hidden.astype(jnp.bfloat16))
    hidden = jnp.concatenate(parts, axis=1)
    down = down_proj[0].reshape(-1, features)
    partial = jnp.dot(hidden, down, preferred_element_type=jnp.float32).astype(jnp.bfloat16)
    mixed = lax.psum_scatter(partial, "ep", scatter_dimension=0, tiled=True)
    return mixed, load_excess


def solution(mesh):
    in_specs = (
        P("ep", None),
        P(),
        P("ep", None),
        P("ep", None, None, None),
        P("ep", None, None, None),
        P("ep", None, None, None),
    )
    out_specs = (P("ep", None), P())
    return jax.shard_map(
        per_device, mesh=mesh, in_specs=in_specs, out_specs=out_specs, check_vma=False
    )
```
